32 devices in a mesh: ep: 4 (over y, core), fs: 8 (over z, x).
Axes of the slice: x: 2, y: 2, z: 4, core: 2. Of those that a mesh axis runs over, the one named last changes fastest.
Arguments:
- grads: bfloat16 [4, 4, 128, 14336], P('ep', None, 'fs'), may hold values from -64 to 64
- counts: int32 [4, 4], replicated, may hold values from 16 to 2047
- weight: bfloat16 [4, 128, 14336], P('ep', 'fs'), may hold values from -3 to 3
- mom: float32 [4, 128, 14336], P('ep', 'fs'), may hold values from -64 to 64
- second: float32 [4, 128, 14336], P('ep', 'fs'), may hold values from 0.1 to 10
- in_weight: float32 [6, 32], replicated, may hold values from -2.5 to 2.5
- in_bias: float32 [32], replicated, may hold values from -3 to 3
- out_weight: float32 [32, 2], replicated, may hold values from -1 to 1
- out_bias: float32 [2], replicated, may hold values from -3 to 3
Outputs:
- new_weight: bfloat16 [4, 128, 14336], P('ep')
- new_mom: float32 [4, 128, 14336], P('ep', 'fs')
- new_second: float32 [4, 128, 14336], P('ep', 'fs')
The draws below stay inside these ranges and needn't reach their ends.
All inputs are finite; a program needn't handle non-finite values.
Results may differ from the reference program's by a relative error of at most 0.0019.
Values may be sent and summed in bfloat16 or wider, within the bound.
A program may use at most 64 MiB of HBM per device.

```python
import math
import jax
import jax.numpy as jnp
from jax import lax

FF = 14336
EXPERTS = 4
R = 128
HID = 32
FEATS = 6


def scaled_field(key, field_shape, magnitude):
    key_noise, key_cols = jax.random.split(key, 2)
    row_scale = 10.0 ** (jnp.arange(R, dtype=jnp.float32) / R)
    col_scale = jnp.exp(jax.random.uniform(key_cols, (FF,), jnp.float32, 0.0, math.log(10.0)))
    noise_field = jnp.clip(jax.random.normal(key_noise, field_shape, jnp.float32), -6.0, 6.0)
    return magnitude * noise_field * row_scale[:, None] * col_scale


def draw_grads(key, part):
    return scaled_field(jax.random.fold_in(key, 101), (EXPERTS, EXPERTS, R, FF), 0.01).astype(jnp.bfloat16)


def draw_mom(key, part):
    return scaled_field(jax.random.fold_in(key, 202), (EXPERTS, R, FF), 0.01)


def touch_ends(array, stream_key, least, top_value):
    index_at = [jax.random.randint(jax.random.fold_in(stream_key, axis), (), 0, length) for axis, length in enumerate(array.shape)]
    longest = array.shape.index(max(array.shape))
    neighbour = index_at[:longest] + [(index_at[longest] + 1) % array.shape[longest]] + index_at[longest + 1:]
    return array.at[tuple(index_at)].set(least).at[tuple(neighbour)].set(top_value)


def level_of(rng, shape, cuts, smallest, top_value):
    factor_of = 1.0
    for position, shards_of in cuts:
        draws = jax.random.uniform(jax.random.fold_in(jax.random.fold_in(rng, 6), position), (shards_of,), jnp.float32, smallest / len(cuts), top_value / len(cuts))
        factor_of = factor_of * jnp.repeat(jnp.exp(draws), shape[position] // shards_of).reshape((-1,) + (1,) * (len(shape) - 1 - position))
    return factor_of


def noise(stream_key, shape, spread, most, cuts=(), held_as=jnp.bfloat16):
    values = jax.random.normal(stream_key, shape, jnp.float32) * spread
    if len(cuts) > 0:
        values = level_of(stream_key, shape, cuts, -0.22, 0.18) * values
    return jnp.clip(values, min=-most, max=most).astype(held_as)


def setup_inputs(seed: int = 0) -> dict:
    key_list = jax.random.split(jax.random.key(seed), 10)
    return {
        "grads": draw_grads(jax.random.fold_in(key_list[9], 71), 0),
        "counts": touch_ends(jax.random.randint(key_list[1], (EXPERTS, EXPERTS), 16, 2048), jax.random.fold_in(key_list[1], 1), 16, 2047).astype(jnp.int32),
        "weight": noise(key_list[2], (EXPERTS, R, FF), 0.5, 3.0, ((0, 4), (1, 8))),
        "mom": draw_mom(jax.random.fold_in(key_list[9], 71), 0),
        "second": jnp.clip(jnp.exp(math.log(10.0) - 4.6051702 * jax.random.uniform(key_list[4], (EXPERTS, R, FF), jnp.float32) ** level_of(key_list[4], (EXPERTS, R, FF), ((0, 4), (1, 8)), -0.2, 0.2)), 0.1, 10.0),
        "in_weight": noise(key_list[5], (FEATS, HID), FEATS ** -0.5, 2.5, (), jnp.float32),
        "in_bias": noise(key_list[6], (HID,), 0.5, 3.0, (), jnp.float32),
        "out_weight": noise(key_list[7], (HID, 2), HID ** -0.5, 1.0, (), jnp.float32),
        "out_bias": noise(key_list[8], (2,), 0.5, 3.0, (), jnp.float32),
    }


MOMENTUM_DECAY = 0.9
SECOND_DECAY = 0.99
NORM_EPS = 1e-06
ROOT_EPS = 1e-08
STEP_SCALE = 0.2
EXP_SCALE = 0.5

def learned_step(gradient, mom_next, second_next, weight, grad_norm, mom_norm, in_weight, in_bias, out_weight, out_bias):
    inv_root = lax.rsqrt(second_next + ROOT_EPS)
    features = jnp.stack([gradient / grad_norm, mom_next / mom_norm, mom_next * inv_root, gradient * inv_root, weight.astype(jnp.float32), jnp.broadcast_to(jnp.log(mom_norm), gradient.shape)])
    hidden = jax.nn.relu(jnp.einsum('fh,fab->hab', in_weight, features, precision=lax.Precision.HIGHEST) + in_bias[:, None, None])
    outputs = jnp.einsum('hk,hab->kab', out_weight, hidden, precision=lax.Precision.HIGHEST) + out_bias[:, None, None]
    update = STEP_SCALE * outputs[0] * jnp.exp(EXP_SCALE * outputs[1])
    return (weight.astype(jnp.float32) - update).astype(jnp.bfloat16)

def reference(grads, counts, weight, mom, second, in_weight, in_bias, out_weight, out_bias):
    counts_f = counts.astype(jnp.float32)
    totals = lax.optimization_barrier(jnp.sum(counts_f, axis=0))
    shares = counts_f / totals[None, :]

    def per_expert(items):
        expert_grads, expert_shares, expert_weight, expert_mom, expert_second = items
        weighted = (expert_shares[:, None, None] * expert_grads.astype(jnp.float32)).astype(jnp.bfloat16)
        weighted = lax.optimization_barrier(weighted)
        gradient = lax.optimization_barrier(jnp.sum(weighted.astype(jnp.float32), axis=0))
        mom_next = MOMENTUM_DECAY * expert_mom + (1.0 - MOMENTUM_DECAY) * gradient
        second_next = SECOND_DECAY * expert_second + (1.0 - SECOND_DECAY) * gradient * gradient
        entries = gradient.shape[0] * gradient.shape[1]
        grad_norm = jnp.sqrt(jnp.sum(gradient * gradient) / entries + NORM_EPS)
        mom_norm = jnp.sqrt(jnp.sum(mom_next * mom_next) / entries + NORM_EPS)
        updated = learned_step(gradient, mom_next, second_next, expert_weight, grad_norm, mom_norm, in_weight, in_bias, out_weight, out_bias)
        return (updated, mom_next, second_next)
    new_weight, new_mom, new_second = lax.map(per_expert, (jnp.swapaxes(grads, 0, 1), shares.T, weight, mom, second))
    return (new_weight, new_mom, new_second)
```

```python
import functools

import jax
import jax.numpy as jnp
from jax import lax
from jax.experimental import pallas as pl
from jax.experimental.pallas import tpu as pltpu
from jax.sharding import PartitionSpec as P

MOMENTUM_DECAY = 0.9
SECOND_DECAY = 0.99
NORM_EPS = 1e-06
ROOT_EPS = 1e-08
STEP_SCALE = 0.2
EXP_SCALE = 0.5
LANES = 128
MOST_CHUNKS = 8


def largest_divisor(number, most):
    return max(d for d in range(1, most + 1) if number % d == 0)


def tile_width(columns, most):
    return LANES * largest_divisor(columns // LANES, most // LANES)


def remote(src, dst, send_sem, recv_sem, axis, peer):
    return pltpu.make_async_remote_copy(
        src_ref=src,
        dst_ref=dst,
        send_sem=send_sem,
        recv_sem=recv_sem,
        device_id={axis: peer},
        device_id_type=pl.DeviceIdType.MESH,
    )


def kernel(
    groups,
    depth,
    across,
    chunks,
    counts,
    in_weight,
    in_bias,
    out_weight,
    out_bias,
    grads,
    weight,
    mom,
    second,
    gathered,
    mom_out,
    second_out,
    outgoing,
    arrived,
    gradient,
    sums,
    bias,
    grad_send,
    grad_recv,
    sum_send,
    sum_recv,
    row_send,
    row_recv,
):
    shards = depth * across
    rows, columns = mom.shape[1], mom.shape[2]
    units = in_bias.shape[0]
    me_group = lax.axis_index("ep")
    me = lax.axis_index("fs")
    z = me // across
    x = me % across

    barrier = pltpu.get_barrier_semaphore()
    for step in range(1, groups):
        pl.semaphore_signal(
            barrier,
            inc=1,
            device_id={"ep": (me_group + step) % groups},
            device_id_type=pl.DeviceIdType.MESH,
        )
    for step in range(1, shards):
        pl.semaphore_signal(
            barrier,
            inc=1,
            device_id={"fs": (me + step) % shards},
            device_id_type=pl.DeviceIdType.MESH,
        )
    pl.semaphore_wait(barrier, groups - 1 + shards - 1)

    wide = tile_width(columns, 1024)

    def share_of(expert):
        total = counts[0, expert]
        for s in range(1, groups):
            total = total + counts[s, expert]
        mine = jnp.full((1, LANES), counts[me_group, expert].astype(jnp.float32))
        return (mine / jnp.full((1, LANES), total.astype(jnp.float32)))[:, :1]

    sends = []
    order = sorted(range(1, groups), key=lambda step: abs(2 * step - groups))
    for step in order:
        peer = (me_group + step) % groups
        share = share_of(peer)

        def weigh(i, carry, peer=peer, share=share, step=step):
            cols = pl.ds(pl.multiple_of(i * wide, wide), wide)
            value = share * grads[0, peer, :, cols].astype(jnp.float32)
            outgoing[step - 1, :, cols] = value.astype(jnp.bfloat16)
            return carry

        lax.fori_loop(0, columns // wide, weigh, 0)
        copy = remote(
            outgoing.at[step - 1],
            arrived.at[step - 1],
            grad_send.at[step - 1],
            grad_recv.at[step - 1],
            "ep",
            peer,
        )
        copy.start()
        sends.append(copy)
    for copy in sends:
        copy.wait_recv()

    share = share_of(me_group)
    narrow = tile_width(columns, 512)

    def moments(i, carry):
        grad_acc, mom_acc = carry
        cols = pl.ds(pl.multiple_of(i * narrow, narrow), narrow)
        own = (share * grads[0, me_group, :, cols].astype(jnp.float32)).astype(jnp.bfloat16)
        total = own.astype(jnp.float32)
        for s in range(groups - 1):
            total = total + arrived[s, :, cols].astype(jnp.float32)
        mom_next = MOMENTUM_DECAY * mom[0, :, cols] + (1.0 - MOMENTUM_DECAY) * total
        gradient[:, cols] = total
        mom_out[0, :, cols] = mom_next
        second_out[0, :, cols] = (
            SECOND_DECAY * second[0, :, cols] + (1.0 - SECOND_DECAY) * total * total
        )
        return grad_acc + total * total, mom_acc + mom_next * mom_next

    zero = jnp.zeros((rows, narrow), jnp.float32)
    grad_acc, mom_acc = lax.fori_loop(0, columns // narrow, moments, (zero, zero))

    def to_lanes(acc):
        acc = jnp.sum(acc, axis=0, keepdims=True)
        return sum(acc[:, j : j + LANES] for j in range(0, narrow, LANES))

    sums[me, 0:1, :] = to_lanes(grad_acc)
    sums[me, 1:2, :] = to_lanes(mom_acc)
    sum_sends = []
    for step in range(1, shards):
        copy = remote(
            sums.at[me],
            sums.at[me],
            sum_send.at[step - 1],
            sum_recv.at[me],
            "fs",
            (me + step) % shards,
        )
        copy.start()
        sum_sends.append(copy)
    for step in range(1, shards):
        source = (me + step) % shards
        remote(
            sums.at[source],
            sums.at[source],
            sum_send.at[step - 1],
            sum_recv.at[source],
            "fs",
            source,
        ).wait_recv()

    entries = rows * columns * shards
    totals = sums[0]
    for s in range(1, shards):
        totals = totals + sums[s]
    mean = jnp.broadcast_to(jnp.sum(totals, axis=1, keepdims=True) / entries, (2, LANES)) + NORM_EPS
    inverse = lax.rsqrt(mean)
    inv_grad = inverse[0:1, :1]
    inv_mom = inverse[1:2, :1]
    log_mom = jnp.max(0.5 * jnp.log(mean[1:2, :]))
    for h in range(units):
        bias[h] = in_bias[h] + in_weight[5, h] * log_mom

    width = columns // chunks
    tile = tile_width(width, 256)

    def learned_step(cols):
        grad = gradient[:, cols]
        mom_next = mom_out[0, :, cols]
        old = weight[0, :, cols].astype(jnp.float32)
        inv_root = lax.rsqrt(second_out[0, :, cols] + ROOT_EPS)
        features = (
            grad * inv_grad,
            mom_next * inv_mom,
            mom_next * inv_root,
            grad * inv_root,
            old,
        )
        direction = jnp.full(grad.shape, out_bias[0])
        magnitude = jnp.full(grad.shape, out_bias[1])
        for h in range(units):
            hidden = features[0] * in_weight[0, h] + bias[h]
            for f in range(1, len(features)):
                hidden = hidden + features[f] * in_weight[f, h]
            hidden = jnp.maximum(hidden, 0.0)
            direction = direction + hidden * out_weight[h, 0]
            magnitude = magnitude + hidden * out_weight[h, 1]
        update = STEP_SCALE * direction * jnp.exp(EXP_SCALE * magnitude)
        return (old - update).astype(jnp.bfloat16)

    def rows_of(source):
        return pl.ds(pl.multiple_of(source * rows, rows), rows)

    ways = (
        (0, across, z < depth - 1),
        (1, -across, z > 0),
        (2, 1, x < across - 1),
        (3, -1, x > 0),
    )

    def block(source, k, full=False):
        if full:
            return gathered.at[0, rows_of(source), :]
        return gathered.at[0, rows_of(source), pl.ds(pl.multiple_of(k * width, width), width)]

    def send(source, k, which):
        for number, offset, possible in ways:
            if number in which:

                @pl.when(possible)
                def _(number=number, offset=offset):
                    piece = block(source, k)
                    remote(
                        piece,
                        piece,
                        row_send.at[number, source],
                        row_recv.at[source, k],
                        "fs",
                        me + offset,
                    ).start()

    def await_block(source, k):
        piece = block(source, k)
        remote(
            piece, piece, row_send.at[0, source], row_recv.at[source, k], "fs", source
        ).wait_recv()

    def turn(t, carry):
        @pl.when(t < chunks)
        def _():
            def one(i, inner):
                cols = pl.ds(pl.multiple_of(t * width + i * tile, tile), tile)
                gathered[0, rows_of(me), cols] = learned_step(cols)
                return inner

            lax.fori_loop(0, width // tile, one, 0)
            send(me, t, (0, 1, 2, 3))

        for d in range(1, depth):
            live = jnp.logical_and(t >= d, t - d < chunks)

            @pl.when(jnp.logical_and(live, z >= d))
            def _(d=d):
                source = me - d * across
                await_block(source, t - d)
                send(source, t - d, (0, 2, 3))

            @pl.when(jnp.logical_and(live, z + d < depth))
            def _(d=d):
                source = me + d * across
                await_block(source, t - d)
                send(source, t - d, (1, 2, 3))

        for e in range(1, across):
            late = depth - 1 + e
            live = jnp.logical_and(t >= late, t - late < chunks)
            for level in range(depth):

                @pl.when(jnp.logical_and(live, x >= e))
                def _(e=e, late=late, level=level):
                    source = level * across + x - e
                    await_block(source, t - late)
                    send(source, t - late, (2,))

                @pl.when(jnp.logical_and(live, x + e < across))
                def _(e=e, late=late, level=level):
                    source = level * across + x + e
                    await_block(source, t - late)
                    send(source, t - late, (3,))

        return carry

    lax.fori_loop(0, chunks + depth - 1 + across - 1, turn, 0)

    for copy in sends:
        copy.wait_send()
    for copy in sum_sends:
        copy.wait_send()
    for number, _, possible in ways:
        for source in range(shards):
            level, place = source // across, source % across
            used = (
                jnp.logical_and(place == x, level <= z),
                jnp.logical_and(place == x, level >= z),
                place <= x,
                place >= x,
            )[number]

            @pl.when(jnp.logical_and(possible, used))
            def _(number=number, source=source):
                piece = block(source, 0, full=True)
                remote(
                    piece,
                    piece,
                    row_send.at[number, source],
                    row_recv.at[source, 0],
                    "fs",
                    (me + 1) % shards,
                ).wait_send()


def per_device(
    groups, shards, grads, counts, weight, mom, second, in_weight, in_bias, out_weight, out_bias
):
    rows, columns = mom.shape[1], mom.shape[2]
    across = max(d for d in range(1, shards + 1) if shards % d == 0 and d * d <= shards)
    depth = shards // across
    chunks = largest_divisor(columns // LANES, MOST_CHUNKS)
    smem = pl.BlockSpec(memory_space=pltpu.SMEM)
    vmem = pl.BlockSpec(memory_space=pltpu.VMEM)
    return pl.pallas_call(
        functools.partial(kernel, groups, depth, across, chunks),
        out_shape=(
            jax.ShapeDtypeStruct((1, rows * shards, columns), jnp.bfloat16),
            jax.ShapeDtypeStruct(mom.shape, jnp.float32),
            jax.ShapeDtypeStruct(second.shape, jnp.float32),
        ),
        in_specs=[smem] * 5 + [vmem] * 4,
        out_specs=(vmem, vmem, vmem),
        scratch_shapes=[
            pltpu.VMEM((groups - 1, rows, columns), jnp.bfloat16),
            pltpu.VMEM((groups - 1, rows, columns), jnp.bfloat16),
            pltpu.VMEM((rows, columns), jnp.float32),
            pltpu.VMEM((shards, 2, LANES), jnp.float32),
            pltpu.SMEM((in_bias.shape[0],), jnp.float32),
            pltpu.SemaphoreType.DMA((groups - 1,)),
            pltpu.SemaphoreType.DMA((groups - 1,)),
            pltpu.SemaphoreType.DMA((shards - 1,)),
            pltpu.SemaphoreType.DMA((shards,)),
            pltpu.SemaphoreType.DMA((4, shards)),
            pltpu.SemaphoreType.DMA((shards, chunks)),
        ],
        compiler_params=pltpu.CompilerParams(
            collective_id=0, has_side_effects=True, vmem_limit_bytes=48 * 1024 * 1024
        ),
        name="learned_update",
    )(counts, in_weight, in_bias, out_weight, out_bias, grads, weight, mom, second)


def solution(mesh):
    in_specs = (
        P("ep", None, "fs", None),
        P(),
        P("ep", "fs", None),
        P("ep", "fs", None),
        P("ep", "fs", None),
        P(),
        P(),
        P(),
        P(),
    )
    out_specs = (P("ep", None, None), P("ep", "fs", None), P("ep", "fs", None))
    body = functools.partial(per_device, mesh.shape["ep"], mesh.shape["fs"])
    return jax.shard_map(
        body, mesh=mesh, in_specs=in_specs, out_specs=out_specs, check_vma=False
    )
```

```python
import functools

import jax
import jax.numpy as jnp
from jax import lax
from jax.experimental import pallas as pl
from jax.experimental.pallas import tpu as pltpu
from jax.sharding import PartitionSpec as P

MOMENTUM_DECAY = 0.9
SECOND_DECAY = 0.99
NORM_EPS = 1e-06
ROOT_EPS = 1e-08
STEP_SCALE = 0.2
EXP_SCALE = 0.5
LANES = 128
MOST_CHUNKS = 14
MOST_CUTS = 4
LAG = 2
VMEM_BYTES = 67043328


def largest_divisor(number, most):
    return max(d for d in range(1, most + 1) if number % d == 0)


def tile_width(columns, most):
    return LANES * largest_divisor(columns // LANES, most // LANES)


def turned_chunks(depth, across, chunks):
    def load(turned):
        straight = chunks - turned
        on_x = (across - 1) * (depth * straight + turned)
        on_z = (depth - 1) * (straight + across * turned)
        return max(on_x, on_z)

    return min(range(chunks + 1), key=load)


def remote(src, dst, send_sem, recv_sem, axis, peer):
    return pltpu.make_async_remote_copy(
        src_ref=src,
        dst_ref=dst,
        send_sem=send_sem,
        recv_sem=recv_sem,
        device_id={axis: peer},
        device_id_type=pl.DeviceIdType.MESH,
    )


def kernel(
    groups,
    depth,
    across,
    chunks,
    counts_hbm,
    in_weight_hbm,
    in_bias_hbm,
    out_weight_hbm,
    out_bias_hbm,
    grads_hbm,
    weight_hbm,
    mom_hbm,
    second_hbm,
    gathered_hbm,
    mom_hbm_out,
    second_hbm_out,
    counts,
    in_weight,
    in_bias,
    out_weight,
    out_bias,
    grads,
    weight,
    mom,
    second,
    gathered,
    outgoing,
    arrived,
    gradient,
    sums,
    bias,
    small_sem,
    slab_sem,
    param_sem,
    grad_send,
    grad_recv,
    flush_sem,
    state_sem,
    sum_send,
    sum_recv,
    row_send,
    row_recv,
):
    shards = depth * across
    rows, columns = mom.shape
    units = in_bias.shape[0]
    me_group = lax.axis_index("ep")
    me = lax.axis_index("fs")
    z = me // across
    x = me % across

    def peer_of(step):
        return (me_group + step) % groups

    small = [
        pltpu.make_async_copy(src, dst, small_sem.at[i])
        for i, (src, dst) in enumerate(
            (
                (counts_hbm, counts),
                (in_weight_hbm, in_weight),
                (in_bias_hbm, in_bias),
                (out_weight_hbm, out_weight),
                (out_bias_hbm, out_bias),
            )
        )
    ]
    for copy in small:
        copy.start()

    slabs = [
        pltpu.make_async_copy(
            grads_hbm.at[0, peer_of(step)], grads.at[step], slab_sem.at[step]
        )
        for step in range(groups)
    ]
    for copy in slabs[1:] + slabs[:1]:
        copy.start()
    params = [
        pltpu.make_async_copy(src.at[0], dst, param_sem.at[i])
        for i, (src, dst) in enumerate(
            (
                (mom_hbm, mom),
                (second_hbm, second),
                (weight_hbm, weight),
            )
        )
    ]
    for copy in params:
        copy.start()

    barrier = pltpu.get_barrier_semaphore()
    for step in range(1, groups):
        pl.semaphore_signal(
            barrier,
            inc=1,
            device_id={"ep": peer_of(step)},
            device_id_type=pl.DeviceIdType.MESH,
        )
    for step in range(1, shards):
        pl.semaphore_signal(
            barrier,
            inc=1,
            device_id={"fs": (me + step) % shards},
            device_id_type=pl.DeviceIdType.MESH,
        )
    pl.semaphore_wait(barrier, groups - 1 + shards - 1)
    for copy in small:
        copy.wait()

    cuts = grad_recv.shape[1]
    cut = columns // cuts
    narrow = tile_width(cut, 512)

    def cols_of(c, i):
        return pl.ds(pl.multiple_of(c * cut + i * narrow, narrow), narrow)

    def piece_of(c):
        return pl.ds(pl.multiple_of(c * cut, cut), cut)

    def share_of(expert):
        total = counts[0, expert]
        for s in range(1, groups):
            total = total + counts[s, expert]
        mine = jnp.full((1, LANES), counts[me_group, expert].astype(jnp.float32))
        return (mine / jnp.full((1, LANES), total.astype(jnp.float32)))[:, :1]

    shares = [share_of(peer_of(step)) for step in range(groups)]

    def weighted(step, cols):
        value = shares[step] * grads[step, :, cols].astype(jnp.float32)
        return value.astype(jnp.bfloat16)

    def grad_copy(step, c):
        return remote(
            outgoing.at[step - 1, :, piece_of(c)],
            arrived.at[step - 1, :, piece_of(c)],
            grad_send.at[step - 1, c],
            grad_recv.at[step - 1, c],
            "ep",
            peer_of(step),
        )

    order = sorted(range(1, groups), key=lambda step: abs(2 * step - groups))
    for copy in slabs:
        copy.wait()

    def send_piece(c, carry):
        for step in order:

            def weigh(i, inner, step=step):
                cols = cols_of(c, i)
                outgoing[step - 1, :, cols] = weighted(step, cols)
                return inner

            lax.fori_loop(0, cut // narrow, weigh, 0)
            grad_copy(step, c).start()
        return carry

    lax.fori_loop(0, cuts, send_piece, 0)
    for copy in params:
        copy.wait()


    def moments(c, carry):
        for step in range(1, groups):
            grad_copy(step, c).wait_recv()

        def one(i, inner):
            grad_acc, mom_acc = inner
            cols = cols_of(c, i)
            total = weighted(0, cols).astype(jnp.float32)
            for step in range(1, groups):
                total = total + arrived[step - 1, :, cols].astype(jnp.float32)
            mom_next = MOMENTUM_DECAY * mom[:, cols] + (1.0 - MOMENTUM_DECAY) * total
            gradient[:, cols] = total
            mom[:, cols] = mom_next
            second[:, cols] = (
                SECOND_DECAY * second[:, cols] + (1.0 - SECOND_DECAY) * total * total
            )
            return grad_acc + total * total, mom_acc + mom_next * mom_next

        return lax.fori_loop(0, cut // narrow, one, carry)

    zero = jnp.zeros((rows, narrow), jnp.float32)
    grad_acc, mom_acc = lax.fori_loop(0, cuts, moments, (zero, zero))

    def to_lanes(acc):
        acc = jnp.sum(acc, axis=0, keepdims=True)
        return sum(acc[:, j : j + LANES] for j in range(0, narrow, LANES))

    sums[me, 0:1, :] = to_lanes(grad_acc)
    sums[me, 1:2, :] = to_lanes(mom_acc)
    sum_sends = []
    for step in range(1, shards):
        copy = remote(
            sums.at[me],
            sums.at[me],
            sum_send.at[step - 1],
            sum_recv.at[me],
            "fs",
            (me + step) % shards,
        )
        copy.start()
        sum_sends.append(copy)
    for step in range(1, shards):
        source = (me + step) % shards
        remote(
            sums.at[source],
            sums.at[source],
            sum_send.at[step - 1],
            sum_recv.at[source],
            "fs",
            source,
        ).wait_recv()

    states = [
        pltpu.make_async_copy(mom, mom_hbm_out.at[0], state_sem.at[0]),
        pltpu.make_async_copy(second, second_hbm_out.at[0], state_sem.at[1]),
    ]
    for copy in states:
        copy.start()

    entries = rows * columns * shards
    totals = sums[0]
    for s in range(1, shards):
        totals = totals + sums[s]
    mean = jnp.broadcast_to(jnp.sum(totals, axis=1, keepdims=True) / entries, (2, LANES)) + NORM_EPS
    inverse = lax.rsqrt(mean)
    inv_grad = inverse[0:1, :1]
    inv_mom = inverse[1:2, :1]
    log_mom = jnp.max(0.5 * jnp.log(mean[1:2, :]))
    for h in range(units):
        bias[h] = in_bias[h] + in_weight[5, h] * log_mom

    width = columns // chunks
    tile = tile_width(width, 256)

    def learned_step(cols):
        grad = gradient[:, cols]
        mom_next = mom[:, cols]
        old = weight[:, cols].astype(jnp.float32)
        inv_root = lax.rsqrt(second[:, cols] + ROOT_EPS)
        features = (
            grad * inv_grad,
            mom_next * inv_mom,
            mom_next * inv_root,
            grad * inv_root,
            old,
        )
        direction = jnp.full(grad.shape, out_bias[0])
        magnitude = jnp.full(grad.shape, out_bias[1])
        for h in range(units):
            hidden = features[0] * in_weight[0, h] + bias[h]
            for f in range(1, len(features)):
                hidden = hidden + features[f] * in_weight[f, h]
            hidden = jnp.maximum(hidden, 0.0)
            direction = direction + hidden * out_weight[0, h]
            magnitude = magnitude + hidden * out_weight[1, h]
        update = STEP_SCALE * direction * jnp.exp(EXP_SCALE * magnitude)
        return (old - update).astype(jnp.bfloat16)

    def rows_of(source):
        return pl.ds(pl.multiple_of(source * rows, rows), rows)

    ways = (
        (across, z < depth - 1),
        (-across, z > 0),
        (1, x < across - 1),
        (-1, x > 0),
    )
    turned = turned_chunks(depth, across, chunks)
    along_z = (z, depth, across, (0, 1))
    along_x = (x, across, 1, (2, 3))
    trees = ((along_x, along_z, 0, turned), (along_z, along_x, turned, chunks))

    def block(source, k):
        return gathered.at[rows_of(source), pl.ds(pl.multiple_of(k * width, width), width)]

    def send(tree, source, k, which):
        for number in which:
            offset, possible = ways[number]

            @pl.when(possible)
            def _(number=number, offset=offset):
                piece = block(source, k)
                remote(
                    piece,
                    piece,
                    row_send.at[tree, number, source],
                    row_recv.at[source, k],
                    "fs",
                    me + offset,
                ).start()

    def flush(source, k):
        cols = pl.ds(pl.multiple_of(k * width, width), width)
        pltpu.make_async_copy(
            block(source, k), gathered_hbm.at[0, rows_of(source), cols], flush_sem.at[source]
        ).start()

    def await_block(source, k):
        piece = block(source, k)
        remote(
            piece, piece, row_send.at[0, 0, source], row_recv.at[source, k], "fs", source
        ).wait_recv()

    def relay(t, tree):
        first, second, low, high = trees[tree]
        if low == high:
            return
        at, size, stride, (up, down) = first
        for d in range(1, size):
            k = t - LAG * d
            live = jnp.logical_and(k >= low, k < high)

            @pl.when(jnp.logical_and(live, at >= d))
            def _(d=d, k=k):
                source = me - d * stride
                await_block(source, k)
                send(tree, source, k, (up,) + second[3])
                flush(source, k)

            @pl.when(jnp.logical_and(live, at + d < size))
            def _(d=d, k=k):
                source = me + d * stride
                await_block(source, k)
                send(tree, source, k, (down,) + second[3])
                flush(source, k)

        other, length, pitch, (up_other, down_other) = second
        for e in range(1, length):
            k = t - LAG * (size - 1 + e)
            live = jnp.logical_and(k >= low, k < high)
            for level in range(size):

                @pl.when(jnp.logical_and(live, other >= e))
                def _(e=e, k=k, level=level):
                    source = level * stride + (other - e) * pitch
                    await_block(source, k)
                    send(tree, source, k, (up_other,))
                    flush(source, k)

                @pl.when(jnp.logical_and(live, other + e < length))
                def _(e=e, k=k, level=level):
                    source = level * stride + (other + e) * pitch
                    await_block(source, k)
                    send(tree, source, k, (down_other,))
                    flush(source, k)

    def turn(t, carry):
        @pl.when(t < chunks)
        def _():
            def one(i, inner):
                cols = pl.ds(pl.multiple_of(t * width + i * tile, tile), tile)
                gathered[rows_of(me), cols] = learned_step(cols)
                return inner

            lax.fori_loop(0, width // tile, one, 0)

        for tree in range(2):
            _, _, low, high = trees[tree]

            @pl.when(jnp.logical_and(t >= low, t < high))
            def _(tree=tree):
                send(tree, me, t, (0, 1, 2, 3))
                flush(me, t)

        for tree in range(2):
            relay(t, tree)
        return carry

    lax.fori_loop(0, chunks + LAG * (depth - 1 + across - 1), turn, 0)

    def drain(c, carry):
        for step in range(1, groups):
            grad_copy(step, c).wait_send()
        return carry

    lax.fori_loop(0, cuts, drain, 0)
    for copy in sum_sends:
        copy.wait_send()
    for copy in states:
        copy.wait()
    for source in range(shards):
        pltpu.make_async_copy(
            gathered.at[rows_of(source), :],
            gathered_hbm.at[0, rows_of(source), :],
            flush_sem.at[source],
        ).wait()
    for tree in range(2):
        first, _, low, high = trees[tree]
        if low == high:
            continue
        for number, (_, possible) in enumerate(ways):
            for source in range(shards):
                level, place = source // across, source % across
                used = (level <= z, level >= z, place <= x, place >= x)[number]
                if first is along_z and number < 2:
                    used = jnp.logical_and(used, place == x)
                if first is along_x and number >= 2:
                    used = jnp.logical_and(used, level == z)

                @pl.when(jnp.logical_and(possible, used))
                def _(tree=tree, number=number, source=source, low=low, high=high):
                    piece = gathered.at[rows_of(source), pl.ds(low * width, (high - low) * width)]
                    remote(
                        piece,
                        piece,
                        row_send.at[tree, number, source],
                        row_recv.at[source, low],
                        "fs",
                        (me + 1) % shards,
                    ).wait_send()


def per_device(
    groups, shards, grads, counts, weight, mom, second, in_weight, in_bias, out_weight, out_bias
):
    rows, columns = mom.shape[1], mom.shape[2]
    across = max(d for d in range(1, shards + 1) if shards % d == 0 and d * d <= shards)
    depth = shards // across
    chunks = largest_divisor(columns // LANES, MOST_CHUNKS)
    cuts = largest_divisor(columns // LANES, MOST_CUTS)
    hbm = pl.BlockSpec(memory_space=pltpu.HBM)
    return pl.pallas_call(
        functools.partial(kernel, groups, depth, across, chunks),
        out_shape=(
            jax.ShapeDtypeStruct((1, rows * shards, columns), jnp.bfloat16),
            jax.ShapeDtypeStruct(mom.shape, jnp.float32),
            jax.ShapeDtypeStruct(second.shape, jnp.float32),
        ),
        in_specs=[hbm] * 9,
        out_specs=(hbm, hbm, hbm),
        scratch_shapes=[
            pltpu.SMEM(counts.shape, jnp.int32),
            pltpu.SMEM(in_weight.shape, jnp.float32),
            pltpu.SMEM(in_bias.shape, jnp.float32),
            pltpu.SMEM(out_weight.shape[::-1], jnp.float32),
            pltpu.SMEM(out_bias.shape, jnp.float32),
            pltpu.VMEM((groups, rows, columns), jnp.bfloat16),
            pltpu.VMEM((rows, columns), jnp.bfloat16),
            pltpu.VMEM((rows, columns), jnp.float32),
            pltpu.VMEM((rows, columns), jnp.float32),
            pltpu.VMEM((rows * shards, columns), jnp.bfloat16),
            pltpu.VMEM((groups - 1, rows, columns), jnp.bfloat16),
            pltpu.VMEM((groups - 1, rows, columns), jnp.bfloat16),
            pltpu.VMEM((rows, columns), jnp.float32),
            pltpu.VMEM((shards, 2, LANES), jnp.float32),
            pltpu.SMEM((in_bias.shape[0],), jnp.float32),
            pltpu.SemaphoreType.DMA((5,)),
            pltpu.SemaphoreType.DMA((groups,)),
            pltpu.SemaphoreType.DMA((3,)),
            pltpu.SemaphoreType.DMA((groups - 1, cuts)),
            pltpu.SemaphoreType.DMA((groups - 1, cuts)),
            pltpu.SemaphoreType.DMA((shards,)),
            pltpu.SemaphoreType.DMA((2,)),
            pltpu.SemaphoreType.DMA((shards - 1,)),
            pltpu.SemaphoreType.DMA((shards,)),
            pltpu.SemaphoreType.DMA((2, 4, shards)),
            pltpu.SemaphoreType.DMA((shards, chunks)),
        ],
        compiler_params=pltpu.CompilerParams(
            collective_id=0, has_side_effects=True, vmem_limit_bytes=VMEM_BYTES
        ),
        name="learned_update",
    )(counts, in_weight, in_bias, out_weight.T, out_bias, grads, weight, mom, second)


def solution(mesh):
    in_specs = (
        P("ep", None, "fs", None),
        P(),
        P("ep", "fs", None),
        P("ep", "fs", None),
        P("ep", "fs", None),
        P(),
        P(),
        P(),
        P(),
    )
    out_specs = (P("ep", None, None), P("ep", "fs", None), P("ep", "fs", None))
    body = functools.partial(per_device, mesh.shape["ep"], mesh.shape["fs"])
    return jax.shard_map(
        body, mesh=mesh, in_specs=in_specs, out_specs=out_specs, check_vma=False
    )
```

```python
import functools

import jax
import jax.numpy as jnp
from jax import lax
from jax.experimental import pallas as pl
from jax.experimental.pallas import tpu as pltpu
from jax.sharding import PartitionSpec as P

MOMENTUM_DECAY = 0.9
SECOND_DECAY = 0.99
NORM_EPS = 1e-06
ROOT_EPS = 1e-08
STEP_SCALE = 0.2
EXP_SCALE = 0.5
LANES = 128
MOST_CHUNKS = 14
MOST_CUTS = 4
LAG = 3
VMEM_BYTES = 67043328


def largest_divisor(number, most):
    return max(d for d in range(1, most + 1) if number % d == 0)


def tile_width(columns, most):
    return LANES * largest_divisor(columns // LANES, most // LANES)


def turned_chunks(depth, across, chunks):
    def load(turned):
        straight = chunks - turned
        on_x = (across - 1) * (depth * straight + turned)
        on_z = (depth - 1) * (straight + across * turned)
        return max(on_x, on_z)

    return min(range(chunks + 1), key=load)


def remote(src, dst, send_sem, recv_sem, axis, peer):
    return pltpu.make_async_remote_copy(
        src_ref=src,
        dst_ref=dst,
        send_sem=send_sem,
        recv_sem=recv_sem,
        device_id={axis: peer},
        device_id_type=pl.DeviceIdType.MESH,
    )


def kernel(
    groups,
    depth,
    across,
    chunks,
    counts_hbm,
    in_weight_hbm,
    in_bias_hbm,
    out_weight_hbm,
    out_bias_hbm,
    grads_hbm,
    weight_hbm,
    mom_hbm,
    second_hbm,
    gathered_hbm,
    mom_hbm_out,
    second_hbm_out,
    counts,
    in_weight,
    in_bias,
    out_weight,
    out_bias,
    grads,
    weight,
    mom,
    second,
    gathered,
    outgoing,
    arrived,
    gradient,
    sums,
    bias,
    small_sem,
    slab_sem,
    param_sem,
    grad_send,
    grad_recv,
    flush_sem,
    state_sem,
    sum_send,
    sum_recv,
    row_send,
    row_recv,
):
    shards = depth * across
    rows, columns = mom.shape
    units = in_bias.shape[0]
    me_group = lax.axis_index("ep")
    me = lax.axis_index("fs")
    z = me // across
    x = me % across

    def peer_of(step):
        return (me_group + step) % groups

    small = [
        pltpu.make_async_copy(src, dst, small_sem.at[i])
        for i, (src, dst) in enumerate(
            (
                (counts_hbm, counts),
                (in_weight_hbm, in_weight),
                (in_bias_hbm, in_bias),
                (out_weight_hbm, out_weight),
                (out_bias_hbm, out_bias),
            )
        )
    ]
    for copy in small:
        copy.start()

    slabs = [
        pltpu.make_async_copy(
            grads_hbm.at[0, peer_of(step)], grads.at[step], slab_sem.at[step]
        )
        for step in range(groups)
    ]
    for copy in slabs[1:] + slabs[:1]:
        copy.start()
    params = [
        pltpu.make_async_copy(src.at[0], dst, param_sem.at[i])
        for i, (src, dst) in enumerate(
            (
                (mom_hbm, mom),
                (second_hbm, second),
                (weight_hbm, weight),
            )
        )
    ]
    for copy in params:
        copy.start()

    barrier = pltpu.get_barrier_semaphore()
    for step in range(1, groups):
        pl.semaphore_signal(
            barrier,
            inc=1,
            device_id={"ep": peer_of(step)},
            device_id_type=pl.DeviceIdType.MESH,
        )
    for step in range(1, shards):
        pl.semaphore_signal(
            barrier,
            inc=1,
            device_id={"fs": (me + step) % shards},
            device_id_type=pl.DeviceIdType.MESH,
        )
    pl.semaphore_wait(barrier, groups - 1 + shards - 1)
    for copy in small:
        copy.wait()

    cuts = grad_recv.shape[1]
    cut = columns // cuts
    narrow = tile_width(cut, 512)

    def cols_of(c, i):
        return pl.ds(pl.multiple_of(c * cut + i * narrow, narrow), narrow)

    def piece_of(c):
        return pl.ds(pl.multiple_of(c * cut, cut), cut)

    def share_of(expert):
        total = counts[0, expert]
        for s in range(1, groups):
            total = total + counts[s, expert]
        mine = jnp.full((1, LANES), counts[me_group, expert].astype(jnp.float32))
        return (mine / jnp.full((1, LANES), total.astype(jnp.float32)))[:, :1]

    shares = [share_of(peer_of(step)) for step in range(groups)]

    def weighted(step, cols):
        value = shares[step] * grads[step, :, cols].astype(jnp.float32)
        return value.astype(jnp.bfloat16)

    def grad_copy(step, c):
        return remote(
            outgoing.at[step - 1, :, piece_of(c)],
            arrived.at[step - 1, :, piece_of(c)],
            grad_send.at[step - 1, c],
            grad_recv.at[step - 1, c],
            "ep",
            peer_of(step),
        )

    order = sorted(range(1, groups), key=lambda step: abs(2 * step - groups))
    for copy in slabs:
        copy.wait()

    def send_piece(c, carry):
        for step in order:

            def weigh(i, inner, step=step):
                cols = cols_of(c, i)
                outgoing[step - 1, :, cols] = weighted(step, cols)
                return inner

            lax.fori_loop(0, cut // narrow, weigh, 0)
            grad_copy(step, c).start()
        return carry

    lax.fori_loop(0, cuts, send_piece, 0)
    for copy in params:
        copy.wait()


    def moments(c, carry):
        for step in range(1, groups):
            grad_copy(step, c).wait_recv()

        def one(i, inner):
            grad_acc, mom_acc = inner
            cols = cols_of(c, i)
            total = weighted(0, cols).astype(jnp.float32)
            for step in range(1, groups):
                total = total + arrived[step - 1, :, cols].astype(jnp.float32)
            mom_next = MOMENTUM_DECAY * mom[:, cols] + (1.0 - MOMENTUM_DECAY) * total
            gradient[:, cols] = total
            mom[:, cols] = mom_next
            second[:, cols] = (
                SECOND_DECAY * second[:, cols] + (1.0 - SECOND_DECAY) * total * total
            )
            return grad_acc + total * total, mom_acc + mom_next * mom_next

        return lax.fori_loop(0, cut // narrow, one, carry)

    zero = jnp.zeros((rows, narrow), jnp.float32)
    grad_acc, mom_acc = lax.fori_loop(0, cuts, moments, (zero, zero))

    def to_lanes(acc):
        acc = jnp.sum(acc, axis=0, keepdims=True)
        return sum(acc[:, j : j + LANES] for j in range(0, narrow, LANES))

    sums[me, 0:1, :] = to_lanes(grad_acc)
    sums[me, 1:2, :] = to_lanes(mom_acc)
    sum_sends = []
    for step in range(1, shards):
        copy = remote(
            sums.at[me],
            sums.at[me],
            sum_send.at[step - 1],
            sum_recv.at[me],
            "fs",
            (me + step) % shards,
        )
        copy.start()
        sum_sends.append(copy)
    for step in range(1, shards):
        source = (me + step) % shards
        remote(
            sums.at[source],
            sums.at[source],
            sum_send.at[step - 1],
            sum_recv.at[source],
            "fs",
            source,
        ).wait_recv()

    states = [
        pltpu.make_async_copy(mom, mom_hbm_out.at[0], state_sem.at[0]),
        pltpu.make_async_copy(second, second_hbm_out.at[0], state_sem.at[1]),
    ]
    for copy in states:
        copy.start()

    entries = rows * columns * shards
    totals = sums[0]
    for s in range(1, shards):
        totals = totals + sums[s]
    mean = jnp.broadcast_to(jnp.sum(totals, axis=1, keepdims=True) / entries, (2, LANES)) + NORM_EPS
    inverse = lax.rsqrt(mean)
    inv_grad = inverse[0:1, :1]
    inv_mom = inverse[1:2, :1]
    log_mom = jnp.max(0.5 * jnp.log(mean[1:2, :]))
    for h in range(units):
        bias[h] = in_bias[h] + in_weight[5, h] * log_mom

    width = columns // chunks
    tile = tile_width(width, 256)

    def learned_step(cols):
        grad = gradient[:, cols]
        mom_next = mom[:, cols]
        old = weight[:, cols].astype(jnp.float32)
        inv_root = lax.rsqrt(second[:, cols] + ROOT_EPS)
        features = (
            grad * inv_grad,
            mom_next * inv_mom,
            mom_next * inv_root,
            grad * inv_root,
            old,
        )
        direction = jnp.full(grad.shape, out_bias[0])
        magnitude = jnp.full(grad.shape, out_bias[1])
        for h in range(units):
            hidden = features[0] * in_weight[0, h] + bias[h]
            for f in range(1, len(features)):
                hidden = hidden + features[f] * in_weight[f, h]
            hidden = jnp.maximum(hidden, 0.0)
            direction = direction + hidden * out_weight[0, h]
            magnitude = magnitude + hidden * out_weight[1, h]
        update = STEP_SCALE * direction * jnp.exp(EXP_SCALE * magnitude)
        return (old - update).astype(jnp.bfloat16)

    def rows_of(source):
        return pl.ds(pl.multiple_of(source * rows, rows), rows)

    ways = (
        (across, z < depth - 1),
        (-across, z > 0),
        (1, x < across - 1),
        (-1, x > 0),
    )
    turned = turned_chunks(depth, across, chunks)
    along_z = (z, depth, across, (0, 1))
    along_x = (x, across, 1, (2, 3))
    trees = ((along_x, along_z, 0, turned), (along_z, along_x, turned, chunks))

    def block(source, k):
        return gathered.at[rows_of(source), pl.ds(pl.multiple_of(k * width, width), width)]

    def send(tree, source, k, which):
        for number in which:
            offset, possible = ways[number]

            @pl.when(possible)
            def _(number=number, offset=offset):
                piece = block(source, k)
                remote(
                    piece,
                    piece,
                    row_send.at[tree, number, source],
                    row_recv.at[source, k],
                    "fs",
                    me + offset,
                ).start()

    def flush(source, k):
        cols = pl.ds(pl.multiple_of(k * width, width), width)
        pltpu.make_async_copy(
            block(source, k), gathered_hbm.at[0, rows_of(source), cols], flush_sem.at[source]
        ).start()

    def await_block(source, k):
        piece = block(source, k)
        remote(
            piece, piece, row_send.at[0, 0, source], row_recv.at[source, k], "fs", source
        ).wait_recv()

    def relay(t, tree):
        first, second, low, high = trees[tree]
        if low == high:
            return
        at, size, stride, (up, down) = first
        for d in range(1, size):
            k = t - LAG * d
            live = jnp.logical_and(k >= low, k < high)

            @pl.when(jnp.logical_and(live, at >= d))
            def _(d=d, k=k):
                source = me - d * stride
                await_block(source, k)
                send(tree, source, k, (up,) + second[3])
                flush(source, k)

            @pl.when(jnp.logical_and(live, at + d < size))
            def _(d=d, k=k):
                source = me + d * stride
                await_block(source, k)
                send(tree, source, k, (down,) + second[3])
                flush(source, k)

        other, length, pitch, (up_other, down_other) = second
        for e in range(1, length):
            k = t - LAG * (size - 1 + e)
            live = jnp.logical_and(k >= low, k < high)
            for level in range(size):

                @pl.when(jnp.logical_and(live, other >= e))
                def _(e=e, k=k, level=level):
                    source = level * stride + (other - e) * pitch
                    await_block(source, k)
                    send(tree, source, k, (up_other,))
                    flush(source, k)

                @pl.when(jnp.logical_and(live, other + e < length))
                def _(e=e, k=k, level=level):
                    source = level * stride + (other + e) * pitch
                    await_block(source, k)
                    send(tree, source, k, (down_other,))
                    flush(source, k)

    def turn(t, carry):
        @pl.when(t < chunks)
        def _():
            def one(i, inner):
                cols = pl.ds(pl.multiple_of(t * width + i * tile, tile), tile)
                gathered[rows_of(me), cols] = learned_step(cols)
                return inner

            lax.fori_loop(0, width // tile, one, 0)

        for tree in range(2):
            _, _, low, high = trees[tree]

            @pl.when(jnp.logical_and(t >= low, t < high))
            def _(tree=tree):
                send(tree, me, t, (0, 1, 2, 3))
                flush(me, t)

        for tree in range(2):
            relay(t, tree)
        return carry

    lax.fori_loop(0, chunks + LAG * (depth - 1 + across - 1), turn, 0)

    def drain(c, carry):
        for step in range(1, groups):
            grad_copy(step, c).wait_send()
        return carry

    lax.fori_loop(0, cuts, drain, 0)
    for copy in sum_sends:
        copy.wait_send()
    for copy in states:
        copy.wait()
    for source in range(shards):
        pltpu.make_async_copy(
            gathered.at[rows_of(source), :],
            gathered_hbm.at[0, rows_of(source), :],
            flush_sem.at[source],
        ).wait()
    for tree in range(2):
        first, _, low, high = trees[tree]
        if low == high:
            continue
        for number, (_, possible) in enumerate(ways):
            for source in range(shards):
                level, place = source // across, source % across
                used = (level <= z, level >= z, place <= x, place >= x)[number]
                if first is along_z and number < 2:
                    used = jnp.logical_and(used, place == x)
                if first is along_x and number >= 2:
                    used = jnp.logical_and(used, level == z)

                @pl.when(jnp.logical_and(possible, used))
                def _(tree=tree, number=number, source=source, low=low, high=high):
                    piece = gathered.at[rows_of(source), pl.ds(low * width, (high - low) * width)]
                    remote(
                        piece,
                        piece,
                        row_send.at[tree, number, source],
                        row_recv.at[source, low],
                        "fs",
                        (me + 1) % shards,
                    ).wait_send()


def per_device(
    groups, shards, grads, counts, weight, mom, second, in_weight, in_bias, out_weight, out_bias
):
    rows, columns = mom.shape[1], mom.shape[2]
    across = max(d for d in range(1, shards + 1) if shards % d == 0 and d * d <= shards)
    depth = shards // across
    chunks = largest_divisor(columns // LANES, MOST_CHUNKS)
    cuts = largest_divisor(columns // LANES, MOST_CUTS)
    hbm = pl.BlockSpec(memory_space=pltpu.HBM)
    return pl.pallas_call(
        functools.partial(kernel, groups, depth, across, chunks),
        out_shape=(
            jax.ShapeDtypeStruct((1, rows * shards, columns), jnp.bfloat16),
            jax.ShapeDtypeStruct(mom.shape, jnp.float32),
            jax.ShapeDtypeStruct(second.shape, jnp.float32),
        ),
        in_specs=[hbm] * 9,
        out_specs=(hbm, hbm, hbm),
        scratch_shapes=[
            pltpu.SMEM(counts.shape, jnp.int32),
            pltpu.SMEM(in_weight.shape, jnp.float32),
            pltpu.SMEM(in_bias.shape, jnp.float32),
            pltpu.SMEM(out_weight.shape[::-1], jnp.float32),
            pltpu.SMEM(out_bias.shape, jnp.float32),
            pltpu.VMEM((groups, rows, columns), jnp.bfloat16),
            pltpu.VMEM((rows, columns), jnp.bfloat16),
            pltpu.VMEM((rows, columns), jnp.float32),
            pltpu.VMEM((rows, columns), jnp.float32),
            pltpu.VMEM((rows * shards, columns), jnp.bfloat16),
            pltpu.VMEM((groups - 1, rows, columns), jnp.bfloat16),
            pltpu.VMEM((groups - 1, rows, columns), jnp.bfloat16),
            pltpu.VMEM((rows, columns), jnp.float32),
            pltpu.VMEM((shards, 2, LANES), jnp.float32),
            pltpu.SMEM((in_bias.shape[0],), jnp.float32),
            pltpu.SemaphoreType.DMA((5,)),
            pltpu.SemaphoreType.DMA((groups,)),
            pltpu.SemaphoreType.DMA((3,)),
            pltpu.SemaphoreType.DMA((groups - 1, cuts)),
            pltpu.SemaphoreType.DMA((groups - 1, cuts)),
            pltpu.SemaphoreType.DMA((shards,)),
            pltpu.SemaphoreType.DMA((2,)),
            pltpu.SemaphoreType.DMA((shards - 1,)),
            pltpu.SemaphoreType.DMA((shards,)),
            pltpu.SemaphoreType.DMA((2, 4, shards)),
            pltpu.SemaphoreType.DMA((shards, chunks)),
        ],
        compiler_params=pltpu.CompilerParams(
            collective_id=0, has_side_effects=True, vmem_limit_bytes=VMEM_BYTES
        ),
        name="learned_update",
    )(counts, in_weight, in_bias, out_weight.T, out_bias, grads, weight, mom, second)


def solution(mesh):
    in_specs = (
        P("ep", None, "fs", None),
        P(),
        P("ep", "fs", None),
        P("ep", "fs", None),
        P("ep", "fs", None),
        P(),
        P(),
        P(),
        P(),
    )
    out_specs = (P("ep", None, None), P("ep", "fs", None), P("ep", "fs", None))
    body = functools.partial(per_device, mesh.shape["ep"], mesh.shape["fs"])
    return jax.shard_map(
        body, mesh=mesh, in_specs=in_specs, out_specs=out_specs, check_vma=False
    )
```
